32 devices in a mesh: occ: 16 (over z, x, core), aux: 2 (over y).
Axes of the slice: x: 2, y: 2, z: 4, core: 2. Of those that a mesh axis runs over, the one named last changes fastest.
Arguments:
- b_factors: bfloat16 [16, 256, 12288], P('occ', None, 'aux'), may hold values from -0.056884766 to 0.056884766
- occ_energies: float32 [16], P('occ'), may hold values from -1.2 to -0.3
- vir_energies: float32 [256], replicated, may hold values from 0.1 to 4
- pair_list: int32 [16, 48, 3], P('occ'), may hold values from -1 to 15, as said below
- pair_count: int32 [16], P('occ'), may hold values from 1 to 48, as said below
Outputs:
- pair_energy: float32 [16, 48], P('occ', 'aux')
- total_energy: float32 [], replicated
The draws below stay inside these ranges and needn't reach their ends.
Inputs may be any that keep to these rules, and one draw needn't show every extreme that they name: `pair_list`: row i lists pair_count[i] distinct items (j, a-block, b-block) with j in 0 to 15 and blocks in 0 to 1, ordered by j, then a-block, then b-block; its other slots hold -1 in all three fields. `pair_count`: some occupied orbital lists exactly 48 items.
All inputs are finite; a program needn't handle non-finite values.
Results may differ from the reference program's by a relative error of at most 0.0003.
Values may be sent and summed in bfloat16 or wider, within the bound.
No kernel may reach another device: no remote copies, remote signals or barrier semaphores. Data moves between devices by JAX's collectives and lax.ppermute only.
A program may use at most 128 MiB of HBM per device.

```python
import math
import jax
import jax.numpy as jnp
from jax import lax

NAUX = 12288
VB = 128
NVB = 2
MAXP = 48
NV = 256
NOCC = 16


def screened_lists(key):
    base_key = jax.random.fold_in(key, 7)
    count_key, full_key, order_key = jax.random.split(base_key, 3)
    lowest = max(MAXP // 2, 1)
    counts = jax.random.randint(count_key, (NOCC,), lowest, MAXP + 1)
    busiest = jax.random.randint(full_key, (), 0, NOCC)
    counts = counts.at[busiest].set(MAXP)
    candidates = NOCC * NVB * NVB

    def choose(order_seed):
        return jax.random.permutation(order_seed, candidates)[:MAXP]
    chosen = jax.vmap(choose)(jax.random.split(order_key, NOCC))
    slot_index = jnp.arange(MAXP, dtype=jnp.int32)
    live_slots = slot_index[None, :] < counts[:, None]
    codes = jnp.sort(jnp.where(live_slots, chosen, candidates), axis=1)
    partner_ids = jnp.where(live_slots, codes // (NVB * NVB), -1)
    left_blocks = jnp.where(live_slots, codes // NVB % NVB, -1)
    right_blocks = jnp.where(live_slots, codes % NVB, -1)
    table = jnp.stack([partner_ids, left_blocks, right_blocks], axis=-1)
    return (table.astype(jnp.int32), counts.astype(jnp.int32))


def draw_pair_list(key, part):
    return screened_lists(key)[0]


def draw_pair_count(key, part):
    return screened_lists(key)[1]


def levels(stream_key, shape, cuts, low, top_value):
    gain = 1.0
    for axis_at, shards_of in cuts:
        heights = jax.random.uniform(jax.random.fold_in(jax.random.fold_in(stream_key, 6), axis_at), (shards_of,), jnp.float32, low / len(cuts), top_value / len(cuts))
        gain = gain * jnp.repeat(jnp.exp(heights), shape[axis_at] // shards_of).reshape((-1,) + (1,) * (len(shape) - 1 - axis_at))
    return gain


def normal_values(stream_key, dims, width, reach, cuts=(), kind=jnp.bfloat16):
    values = width * jax.random.normal(stream_key, dims, jnp.float32)
    if cuts:
        values = values * levels(stream_key, dims, cuts, -0.22, 0.18)
    return jnp.clip(values, -reach, reach).astype(kind)


def setup_inputs(seed: int = 0) -> dict:
    streams_of = jax.random.split(jax.random.key(seed), 6)
    b_factors = normal_values(streams_of[0], (NOCC, NV, NAUX), 0.0095, 0.056884766, ((0, 16), (2, 2)))
    occ_energies = jnp.clip(-1.2 + 0.90000004 * jax.random.uniform(streams_of[1], (NOCC,), jnp.float32) ** levels(streams_of[1], (NOCC,), ((0, 16),), -0.2, 0.2), -1.2, -0.3)
    vir_energies = jnp.clip(jnp.exp(jax.random.uniform(streams_of[2], (NV,), jnp.float32, math.log(0.1), math.log(4.0))), 0.1, 4.0)
    pair_list = draw_pair_list(jax.random.fold_in(streams_of[5], 71), 0)
    pair_count = draw_pair_count(jax.random.fold_in(streams_of[5], 71), 0)
    return dict(b_factors=b_factors, occ_energies=occ_energies, vir_energies=vir_energies, pair_list=pair_list, pair_count=pair_count)


def reference(b_factors, occ_energies, vir_energies, pair_list, pair_count):
    float_factors = b_factors.astype(jnp.float32)

    def one_orbital(packed):
        orbital, entries, listed = packed
        home_panel = lax.dynamic_index_in_dim(float_factors, orbital, 0, keepdims=False)
        home_energy = lax.dynamic_index_in_dim(occ_energies, orbital, 0, keepdims=False)

        def one_item(packed_item):
            slot_index, entry_row = packed_item
            partner_id = jnp.maximum(entry_row[0], 0).astype(jnp.int32)
            left_block = jnp.maximum(entry_row[1], 0).astype(jnp.int32)
            right_block = jnp.maximum(entry_row[2], 0).astype(jnp.int32)
            partner_panel = lax.dynamic_index_in_dim(float_factors, partner_id, 0, keepdims=False)
            home_left = lax.dynamic_slice_in_dim(home_panel, left_block * VB, VB, 0)
            home_right = lax.dynamic_slice_in_dim(home_panel, right_block * VB, VB, 0)
            partner_left = lax.dynamic_slice_in_dim(partner_panel, left_block * VB, VB, 0)
            partner_right = lax.dynamic_slice_in_dim(partner_panel, right_block * VB, VB, 0)
            direct = jnp.dot(home_left, partner_right.T, precision=lax.Precision.HIGHEST)
            swapped = jnp.dot(home_right, partner_left.T, precision=lax.Precision.HIGHEST)
            left_energy = lax.dynamic_slice_in_dim(vir_energies, left_block * VB, VB, 0)
            right_energy = lax.dynamic_slice_in_dim(vir_energies, right_block * VB, VB, 0)
            partner_energy = lax.dynamic_index_in_dim(occ_energies, partner_id, 0, keepdims=False)
            denominator = (left_energy[:, None] + right_energy[None, :]) - home_energy - partner_energy
            energy = -jnp.sum(direct * (2.0 * direct - swapped.T) / denominator)
            return jnp.where(slot_index < listed, energy, jnp.zeros_like(energy))

        return lax.map(one_item, (jnp.arange(MAXP, dtype=jnp.int32), entries))

    pair_energy = lax.map(one_orbital, (jnp.arange(NOCC, dtype=jnp.int32), pair_list, pair_count))
    return pair_energy, jnp.sum(pair_energy)
```

```python
import functools

import jax
import jax.numpy as jnp
import numpy as np
from jax import lax
from jax.experimental import pallas as pl
from jax.experimental.pallas import tpu as pltpu
from jax.sharding import PartitionSpec as P

VB = 128
CORES = 2
LANES = 128


def ring_order(mesh):
    devices = mesh.devices[:, 0]
    chips = len(devices) // CORES
    plain = list(range(chips))
    places = [getattr(d, "coords", None) for d in devices[::CORES]]
    if any(p is None for p in places) or len(set(map(tuple, places))) != chips:
        return plain
    at = {tuple(p): k for k, p in enumerate(places)}
    axes = [sorted({p[d] for p in places}) for d in range(len(places[0]))]
    long = [d for d, values in enumerate(axes) if len(values) > 1]
    if len(long) != 2 or len(axes[long[0]]) * len(axes[long[1]]) != chips:
        return plain
    u, v = sorted(long, key=lambda d: len(axes[d]) % 2)
    if len(axes[u]) % 2:
        return plain

    def chip(i, j):
        place = list(places[0])
        place[u], place[v] = axes[u][i], axes[v][j]
        return at[tuple(place)]

    rows, columns = len(axes[u]), len(axes[v])
    order = []
    for i in range(rows):
        inner = range(1, columns) if i % 2 == 0 else range(columns - 1, 0, -1)
        order += [chip(i, j) for j in inner]
    return order + [chip(i, 0) for i in range(rows - 1, -1, -1)]


def energy_kernel(blocks, ids_ref, occ_ref, vcol_ref, vrow_ref, weight_ref, first_ref, second_ref, base_ref, table_ref):
    rows = lax.broadcasted_iota(jnp.int32, table_ref.shape, 0)
    columns = lax.broadcasted_iota(jnp.int32, table_ref.shape, 1)
    table = base_ref[...]
    pair_sum = vcol_ref[:, :1] + vrow_ref[:1, :]
    for m in range(first_ref.shape[0]):
        i = ids_ref[m, 0]
        j = ids_ref[m, 1]
        tile = first_ref[m] + second_ref[m]
        denominator = pair_sum - occ_ref[i] - occ_ref[j]
        terms = tile * (2.0 * tile - jnp.transpose(tile)) / denominator
        for a in range(blocks):
            line = jnp.sum(terms[a * VB : (a + 1) * VB], axis=0, keepdims=True)
            for b in range(blocks):
                value = -weight_ref[m] * jnp.sum(line[:, b * VB : (b + 1) * VB], axis=1, keepdims=True)
                here = (rows == i) & (columns == (j * blocks + a) * blocks + b)
                there = (rows == j) & (columns == (i * blocks + b) * blocks + a)
                table += jnp.where(here, value, 0.0) + jnp.where(there, value, 0.0)
    table_ref[...] = table


def add_energies(blocks, ids, occ, vcol, vrow, weights, first, second, base):
    smem = pl.BlockSpec(memory_space=pltpu.SMEM)
    vmem = pl.BlockSpec(memory_space=pltpu.VMEM)
    return pl.pallas_call(
        functools.partial(energy_kernel, blocks),
        out_shape=jax.ShapeDtypeStruct(base.shape, jnp.float32),
        in_specs=[smem, smem, vmem, vmem, smem, vmem, vmem, vmem],
        out_specs=vmem,
        cost_estimate=pl.CostEstimate(
            flops=20 * first.size, bytes_accessed=8 * first.size, transcendentals=0
        ),
    )(ids, occ, vcol, vrow, weights, first, second, base)


def sum_over(value, names):
    for name in names:
        size = lax.axis_size(name)
        if size & (size - 1):
            value = lax.psum(value, name)
            continue
        step = 1
        while step < size:
            value = value + lax.ppermute(value, name, [(k, k ^ step) for k in range(size)])
            step *= 2
    return value


def product(left, right):
    return lax.dot_general(left, right, (((1,), (1,)), ((), ())), preferred_element_type=jnp.float32)


def local(order, b_factors, occ_energies, vir_energies, pair_list, pair_count):
    panel = b_factors[0]
    virt, depth = panel.shape
    blocks = virt // VB
    occ_size = lax.axis_size("occ")
    aux_size = lax.axis_size("aux")
    me = lax.axis_index("occ")
    my_aux = lax.axis_index("aux")
    core = me % CORES
    chips = occ_size // CORES
    place = {c: k for k, c in enumerate(order)}

    items = pair_list[0]
    slots = items.shape[0]
    codes = (items[:, 0] * blocks + items[:, 1]) * blocks + items[:, 2]
    live = jnp.arange(slots, dtype=jnp.int32) < pair_count[0]
    width = -(-(occ_size * blocks * blocks) // LANES) * LANES
    code_ids = jnp.arange(width, dtype=jnp.int32)
    listed = jnp.sum(((codes[:, None] == code_ids[None, :]) & live[:, None]).astype(jnp.float32), axis=0)
    facts = jnp.concatenate([listed, jnp.broadcast_to(occ_energies, (LANES,))])
    mine = (jnp.arange(occ_size, dtype=jnp.int32) == me)[:, None]
    facts = sum_over(jnp.where(mine, facts[None, :], 0.0), ["occ"])
    listed_all = facts[:, :width]
    occ_all = facts[:, width]

    share = depth // CORES
    swap = [(k, k ^ 1) for k in range(occ_size)]

    def turn(step):
        return [
            (c * CORES + k, order[(place[c] + step) % chips] * CORES + k)
            for c in range(chips)
            for k in range(CORES)
        ]

    kept = lax.dynamic_slice_in_dim(panel, core * share, share, 1)
    sent = lax.dynamic_slice_in_dim(panel, (1 - core) * share, share, 1)
    got = lax.ppermute(sent, "occ", swap)
    home = [kept[b * VB : (b + 1) * VB] for b in range(blocks)]
    home += [got[b * VB : (b + 1) * VB] for b in range(blocks)]

    hops = -(-(chips // 2) // 2)
    held = {0: home}
    up, down = turn(1), turn(-1)
    for hop in range(1, hops + 1):
        below, above = [], []
        for k in range(len(home)):
            below.append(lax.ppermute(held[1 - hop][k], "occ", up))
            above.append(lax.ppermute(held[hop - 1][k], "occ", down))
        held[-hop], held[hop] = below, above
    slabs = {k: jnp.concatenate(v, axis=0) for k, v in held.items()}

    ring_ids = jnp.asarray(
        np.array([[order[(place[c] + o) % chips] for o in range(-hops, hops + 1)] for c in range(chips)], np.int32)
    )[me // CORES]
    virt_col = jnp.broadcast_to(vir_energies[:, None], (virt, LANES))
    virt_row = jnp.broadcast_to(vir_energies[None, :], (8, virt))

    def work(distance):
        a = -(distance // 2)
        b = a + distance
        whole = product(slabs[a], slabs[b])
        other = lax.ppermute(whole[virt:], "occ", swap)
        weight = 0.5 if distance == 0 or 2 * distance == chips else 1.0
        own = [whole[:virt, :virt], whole[:virt, virt:]]
        other = [other[:, virt:], other[:, :virt]]
        i = ring_ids[a + hops] * CORES + core
        js = [ring_ids[b + hops] * CORES + core, ring_ids[b + hops] * CORES + 1 - core]
        both = [x + y for x, y in zip(own, other)]
        if aux_size == 2:
            first = my_aux == 0
            keep = jnp.where(first, both[0], both[1])
            send = jnp.where(first, both[1], both[0])
            return [(i, jnp.where(first, js[0], js[1]), weight, keep, lax.ppermute(send, "aux", [(0, 1), (1, 0)]))]
        both = [lax.psum(x, "aux") for x in both]
        return [(i, j, weight / aux_size, x, jnp.zeros_like(x)) for j, x in zip(js, both)]

    table = jnp.zeros((occ_size, width), jnp.float32)
    distances = list(range(chips // 2 + 1))
    early = [d for d in distances if d <= 2 * (hops - 1)]
    late = [d for d in distances if d not in early]
    for group in (early, late):
        done = [x for d in group for x in work(d)]
        ids = jnp.stack([jnp.stack([x[0], x[1]]) for x in done]).astype(jnp.int32)
        weights = jnp.asarray(np.array([x[2] for x in done], np.float32))
        first = jnp.stack([x[3] for x in done])
        second = jnp.stack([x[4] for x in done])
        table = add_energies(blocks, ids, occ_all, virt_col, virt_row, weights, first, second, table)
    table = sum_over(table, ["occ", "aux"])

    per_device = slots // aux_size
    my_codes = lax.dynamic_slice_in_dim(codes, my_aux * per_device, per_device, 0)
    my_live = lax.dynamic_slice_in_dim(live, my_aux * per_device, per_device, 0)
    row = jnp.sum(jnp.where(mine, table, 0.0), axis=0)
    energy = jnp.sum(jnp.where(my_codes[:, None] == code_ids[None, :], row[None, :], 0.0), axis=1)
    energy = jnp.where(my_live, energy, 0.0)
    total = jnp.sum(table * listed_all)
    return energy[None, :], total


def solution(mesh):
    return jax.shard_map(
        functools.partial(local, ring_order(mesh)),
        mesh=mesh,
        in_specs=(P("occ", None, "aux"), P("occ"), P(), P("occ", None, None), P("occ")),
        out_specs=(P("occ", "aux"), P()),
        check_vma=False,
    )
```

```python
import functools

import jax
import jax.numpy as jnp
import numpy as np
from jax import lax
from jax.experimental import pallas as pl
from jax.experimental.pallas import tpu as pltpu
from jax.sharding import PartitionSpec as P

VB = 128
CORES = 2
LANES = 128


def ring_order(mesh):
    devices = mesh.devices[:, 0]
    chips = len(devices) // CORES
    plain = list(range(chips))
    places = [getattr(d, "coords", None) for d in devices[::CORES]]
    if any(p is None for p in places) or len(set(map(tuple, places))) != chips:
        return plain
    at = {tuple(p): k for k, p in enumerate(places)}
    axes = [sorted({p[d] for p in places}) for d in range(len(places[0]))]
    long = [d for d, values in enumerate(axes) if len(values) > 1]
    if len(long) != 2 or len(axes[long[0]]) * len(axes[long[1]]) != chips:
        return plain
    u, v = sorted(long, key=lambda d: len(axes[d]) % 2)
    if len(axes[u]) % 2:
        return plain

    def chip(i, j):
        place = list(places[0])
        place[u], place[v] = axes[u][i], axes[v][j]
        return at[tuple(place)]

    rows, columns = len(axes[u]), len(axes[v])
    order = []
    for i in range(rows):
        inner = range(1, columns) if i % 2 == 0 else range(columns - 1, 0, -1)
        order += [chip(i, j) for j in inner]
    return order + [chip(i, 0) for i in range(rows - 1, -1, -1)]


def energy_kernel(blocks, ids_ref, occ_ref, vcol_ref, vrow_ref, weight_ref, first_ref, second_ref, base_ref, table_ref):
    rows = lax.broadcasted_iota(jnp.int32, table_ref.shape, 0)
    columns = lax.broadcasted_iota(jnp.int32, table_ref.shape, 1)
    table = base_ref[...]
    pair_sum = vcol_ref[:, :1] + vrow_ref[:1, :]
    for m in range(first_ref.shape[0]):
        i = ids_ref[m, 0]
        j = ids_ref[m, 1]
        tile = first_ref[m] + second_ref[m]
        denominator = pair_sum - occ_ref[i] - occ_ref[j]
        terms = tile * (2.0 * tile - jnp.transpose(tile)) / denominator
        for a in range(blocks):
            line = jnp.sum(terms[a * VB : (a + 1) * VB], axis=0, keepdims=True)
            for b in range(blocks):
                value = -weight_ref[m] * jnp.sum(line[:, b * VB : (b + 1) * VB], axis=1, keepdims=True)
                here = (rows == i) & (columns == (j * blocks + a) * blocks + b)
                there = (rows == j) & (columns == (i * blocks + b) * blocks + a)
                table += jnp.where(here, value, 0.0) + jnp.where(there, value, 0.0)
    table_ref[...] = table


def add_energies(blocks, ids, occ, vcol, vrow, weights, first, second, base):
    smem = pl.BlockSpec(memory_space=pltpu.SMEM)
    vmem = pl.BlockSpec(memory_space=pltpu.VMEM)
    return pl.pallas_call(
        functools.partial(energy_kernel, blocks),
        out_shape=jax.ShapeDtypeStruct(base.shape, jnp.float32),
        in_specs=[smem, smem, vmem, vmem, smem, vmem, vmem, vmem],
        out_specs=vmem,
        cost_estimate=pl.CostEstimate(
            flops=20 * first.size, bytes_accessed=8 * first.size, transcendentals=0
        ),
    )(ids, occ, vcol, vrow, weights, first, second, base)


NEAR = {
    "HH": ("H", "H", 0.5),
    "HB": ("H", "B", 1.0),
    "HX": ("H", "X", 0.5),
    "BA": ("B", "A", 1.0),
    "BX": ("B", "X", 1.0),
}
FAR = {
    "FU": ("F", "U", "same", "FU"),
    "FX": ("F", "X", "cross", "LG"),
    "LG": ("L", "G", "cross", "FX"),
    "FG": ("F", "G", "cross", "FG"),
}
KINDS = ("same", "cross")
SLOTS = ("H", "X", "L", "U", "F", "G")
TAIL = 8


def grid_of(mesh):
    devices = mesh.devices[:, 0]
    places = [getattr(d, "coords", None) for d in devices[::CORES]]
    if any(p is None for p in places) or len(devices) % CORES:
        return None
    axes = [sorted({p[d] for p in places}) for d in range(len(places[0]))]
    long = sorted((d for d, v in enumerate(axes) if len(v) > 1), key=lambda d: len(axes[d]))
    if [len(axes[d]) for d in long] != [2, 4] or len(set(map(tuple, places))) != len(places):
        return None
    return [(axes[long[0]].index(p[long[0]]), axes[long[1]].index(p[long[1]])) for p in places]


def split_kernel(extra, offset_ref, panel_ref, tail_ref, kept_ref, sent_ref, sems):
    rows, share = kept_ref.shape
    copies = []
    for n, target in enumerate((sent_ref, kept_ref)):
        start = pl.multiple_of(offset_ref[1 - n] * share, LANES)
        source = panel_ref.at[extra, pl.ds(start, share)]
        copies.append(pltpu.make_async_copy(source, target.at[pl.ds(0, rows)], sems.at[n]))
        copies[-1].start()
    if sent_ref.shape[0] > rows:
        sent_ref[rows:] = tail_ref[...]
    for copy in copies:
        copy.wait()


def split(panel, block, cores, tail, share):
    smem = pl.BlockSpec(memory_space=pltpu.SMEM)
    vmem = pl.BlockSpec(memory_space=pltpu.VMEM)
    below = tail.shape[0] if block == 0 else 0
    return pl.pallas_call(
        functools.partial(split_kernel, pl.ds(block * VB, VB)),
        out_shape=(
            jax.ShapeDtypeStruct((VB, share), panel.dtype),
            jax.ShapeDtypeStruct((VB + below, share), panel.dtype),
        ),
        in_specs=[smem, pl.BlockSpec(memory_space=pltpu.HBM), vmem],
        out_specs=(vmem, vmem),
        scratch_shapes=[pltpu.SemaphoreType.DMA((2,))],
        compiler_params=pltpu.CompilerParams(vmem_limit_bytes=8 << 20),
    )(cores, panel, tail)


def product_kernel(steps, picks, row_ref, aux_ref, *refs):
    keep_ref, send_ref = refs[-2:]
    core = row_ref[0, 0]
    aux = aux_ref[0]
    diag = (aux + core) % CORES == 0
    plain = aux == 0

    def run(left, right, unit):
        block = lax.dot_general(
            refs[left][: CORES * VB], refs[right][: CORES * VB], (((1,), (1,)), ((), ())), preferred_element_type=jnp.float32
        )
        half = VB
        t00, t01 = block[:half, :half], block[:half, half:]
        t10, t11 = block[half:, :half], block[half:, half:]
        if picks:
            keep_ref[0, unit] = jnp.where(diag, t00, t11)
            send_ref[0, unit] = jnp.where(diag, t11, t00)
            keep_ref[1, unit] = jnp.where(plain, t10, t01)
            send_ref[1, unit] = jnp.where(plain, t01, t10)
        else:
            keep_ref[0, unit], keep_ref[1, unit] = t00, t01
            send_ref[0, unit], send_ref[1, unit] = t11, t10

    for unit, options in enumerate(steps):
        if len(options) == 1:
            run(*options[0], unit)
        else:
            for k, option in enumerate(options):
                pl.when(core == k)(functools.partial(run, *option, unit))


def products(units, chunks, row, aux, picks):
    arrays, places, steps = [], {}, []

    def place(name):
        if name not in places:
            places[name] = len(arrays)
            arrays.append(chunks[name])
        return places[name]

    for unit in units:
        options = []
        for k in range(CORES):
            option = tuple(place(chunks[c][k] if isinstance(chunks[c], tuple) else c) for c in unit)
            options += [option] if option not in options else []
        steps.append(options)
    rows, depth = CORES * VB, arrays[0].shape[1]
    count = len(units)
    dims = (2, count, VB, VB)
    smem = pl.BlockSpec(memory_space=pltpu.SMEM)
    vmem = pl.BlockSpec(memory_space=pltpu.VMEM)
    return pl.pallas_call(
        functools.partial(product_kernel, steps, picks),
        out_shape=(jax.ShapeDtypeStruct(dims, jnp.float32),) * 2,
        in_specs=[smem, smem] + [vmem] * len(arrays),
        out_specs=(vmem, vmem),
        compiler_params=pltpu.CompilerParams(vmem_limit_bytes=30 << 20),
        cost_estimate=pl.CostEstimate(
            flops=2 * rows * rows * depth * count, bytes_accessed=2 * len(arrays) * rows * depth, transcendentals=0
        ),
    )(row, aux, *arrays)


def tile_kernel(blocks, tiles, based, row_ref, aux_ref, vir_ref, occ_ref, *refs):
    table_ref = refs[-1]
    arrays = refs[1:-1] if based else refs[:-1]
    rows = lax.broadcasted_iota(jnp.int32, table_ref.shape, 0)
    columns = lax.broadcasted_iota(jnp.int32, table_ref.shape, 1)
    table = refs[0][...] if based else jnp.zeros(table_ref.shape, jnp.float32)
    aux, core = aux_ref[0], row_ref[0, 0]
    mixed = (aux + core) % CORES
    line = [vir_ref[:, a * VB : (a + 1) * VB] for a in range(blocks)]
    tall = [jnp.transpose(jnp.broadcast_to(x, (VB, VB))) for x in line]
    for place, scale, sides, parts in tiles:
        offset = {"far": (aux, mixed), "near": (core, mixed)}[sides]
        i = row_ref[0, place] * CORES + offset[0]
        j = row_ref[0, place + 1] * CORES + offset[1]
        left_energy = occ_ref[pl.ds(row_ref[0, place + 3] * CORES + (offset[0] + core) % CORES, 1), :]
        right_energy = occ_ref[pl.ds(row_ref[0, place + 4] * CORES + (offset[1] + core) % CORES, 1), :]
        weight = row_ref[0, place + 2].astype(jnp.float32) * -scale
        tile = {}
        for key, (one, u, two, w, turned) in parts.items():
            other = arrays[two][w]
            tile[key] = arrays[one][u] + (jnp.transpose(other) if turned else other)
        for a in range(blocks):
            for b in range(blocks):
                denominator = (tall[a] + line[b]) - left_energy - right_energy
                terms = tile[a, b] * (2.0 * tile[a, b] - jnp.transpose(tile[b, a])) / denominator
                value = weight * jnp.sum(jnp.sum(terms, axis=0, keepdims=True), axis=1, keepdims=True)
                here = (rows == i) & (columns == (j * blocks + a) * blocks + b)
                there = (rows == j) & (columns == (i * blocks + b) * blocks + a)
                table += jnp.where(here, value, 0.0) + jnp.where(there, value, 0.0)
    table_ref[...] = table


def add_tiles(blocks, tiles, row, aux, vir, occ, base, shape, arrays):
    smem = pl.BlockSpec(memory_space=pltpu.SMEM)
    vmem = pl.BlockSpec(memory_space=pltpu.VMEM)
    given = [] if base is None else [base]
    size = len(tiles) * (blocks * VB) ** 2
    return pl.pallas_call(
        functools.partial(tile_kernel, blocks, tiles, base is not None),
        out_shape=jax.ShapeDtypeStruct(shape, jnp.float32),
        in_specs=[smem, smem] + [vmem] * (2 + len(given) + len(arrays)),
        out_specs=vmem,
        compiler_params=pltpu.CompilerParams(vmem_limit_bytes=16 << 20),
        cost_estimate=pl.CostEstimate(flops=40 * size, bytes_accessed=8 * size, transcendentals=0),
    )(row, aux, vir, occ, *given, *arrays)


def two_way(grid, panel, my_energy, vir_energies, shape):
    virt, depth = panel.shape
    blocks = virt // VB
    occ_size = lax.axis_size("occ")
    aux_size = lax.axis_size("aux")
    me = lax.axis_index("occ")
    my_aux = lax.axis_index("aux")
    core = me % CORES
    share = depth // CORES
    chip_at = {p: c for c, p in enumerate(grid)}
    last = max(p[1] for p in grid)

    def row_of(role, k):
        return role if k == 0 else last - role

    def device(u, role, k):
        return chip_at[u, row_of(role, k)] * CORES + k

    every = [(u, k) for u in range(2) for k in range(CORES)]
    ahead = [(device(u, r, k), device(u, r + 1, k)) for u, k in every for r in range(last)]
    back = [(device(u, r + 1, k), device(u, r, k)) for u, k in every for r in range(last)]
    across = [(device(u, r, k), device(1 - u, r, k)) for u, k in every for r in range(last + 1)]
    far_ahead = [(device(u, 1, k), device(u, 2, k)) for u, k in every]
    far_across = [(device(u, 2, k), device(1 - u, 2, k)) for u, k in every]
    swap = [(k, k ^ 1) for k in range(occ_size)]
    centres = sorted(device(u, 2, k) for u, k in every)
    over_aux = [(d * aux_size + y, d * aux_size + 1 - y) for d in centres for y in range(aux_size)]
    all_aux = [(y, 1 - y) for y in range(aux_size)]
    partner = {
        "same": [(device(u, 2, k), device(u, 2, 1 - k)) for u, k in every],
        "cross": [(device(u, 2, k), device(1 - u, 2, 1 - k)) for u, k in every],
    }

    line = lax.broadcasted_iota(jnp.int32, (TAIL, share), 0)
    rest = jnp.broadcast_to(my_energy[:, None], (TAIL, share))
    tail = jnp.zeros((TAIL, share), jnp.float32)
    for n in range(3):
        term = lax.reduce_precision(rest, 8, 7)
        tail = jnp.where(line == n, term, tail)
        rest = rest - term
    tail = tail.astype(panel.dtype)
    cores = jnp.stack([core, 1 - core]).astype(jnp.int32)
    chunks = {}
    for b in range(blocks):
        kept, sent = split(panel, b, cores, tail, share)
        got = lax.ppermute(sent, "occ", swap)
        pieces = [kept, got[:VB], tail, got[VB:]] if b == 0 else [kept, got]
        home = jnp.concatenate(pieces, axis=0)
        chunks["H", b] = home
        chunks["L", b] = lax.ppermute(home, "occ", ahead)
        chunks["U", b] = lax.ppermute(home, "occ", back)
        chunks["X", b] = lax.ppermute(home, "occ", across)
    for b in range(blocks):
        chunks["F", b] = lax.ppermute(chunks["L", b], "occ", far_ahead)
        chunks["G", b] = lax.ppermute(chunks["U", b], "occ", far_across)
        chunks["B", b] = (("L", b), ("U", b))
        chunks["A", b] = (("U", b), ("L", b))

    facts = []
    for d in range(occ_size):
        (u, v), k = grid[d // CORES], d % CORES
        r = row_of(v, k)
        places = {"H": (u, v), "B": (u, v - 1), "A": (u, v + 1), "X": (1 - u, v)}
        places |= {"F": (u, row_of(0, k)), "L": (u, row_of(1, k)), "U": (u, row_of(3, k)), "G": (1 - u, row_of(3, k))}
        line = [k]
        slot = {n: n for n in SLOTS} | {"B": "LU"[k], "A": "UL"[k]}
        for table in (NEAR, FAR):
            for left, right in [x[:2] for x in table.values()]:
                good = places[left] in chip_at and places[right] in chip_at if table is NEAR else r == 2
                line += [chip_at.get(places[left], 0), chip_at.get(places[right], 0), int(good)]
                line += [SLOTS.index(slot[left]), SLOTS.index(slot[right])]
        facts.append(line)
    row = lax.dynamic_slice_in_dim(jnp.asarray(np.array(facts, np.int32)), me, 1, 0)
    aux = jnp.reshape(my_aux, (1,)).astype(jnp.int32)

    def at(name, b):
        return {"H": 0, "F": blocks + b, "G": blocks + b}.get(name, b)

    arrays, where_own, where_other = [], {}, {}

    def units_of(table, event):
        return [
            (name, a, b)
            for name, spec in table.items()
            for a in range(blocks)
            for b in range(blocks)
            if max(at(spec[0], a), at(spec[1], b)) == event
        ]

    upper = my_aux == 0
    for event in range(blocks):
        units = units_of(NEAR, event)
        work = [((NEAR[name][0], a), (NEAR[name][1], b)) for name, a, b in units]
        keep, send = products(work, chunks, row, aux, False)
        keep = keep + lax.ppermute(send, "occ", swap)
        other = lax.ppermute(jnp.where(upper, keep[1], keep[0]), "aux", all_aux)
        for n, unit in enumerate(units):
            where_own[unit] = (len(arrays), n)
            where_other[unit] = (len(arrays) + 1, n)
        arrays += [jnp.where(upper, keep[0], keep[1]), other]
    for event in range(blocks, 2 * blocks):
        units = sorted(units_of(FAR, event), key=lambda u: KINDS.index(FAR[u[0]][2]))
        work = [((FAR[name][0], a), (FAR[name][1], b)) for name, a, b in units]
        keep, send = products(work, chunks, row, aux, True)
        keep = keep + lax.ppermute(send, ("occ", "aux"), over_aux)
        theirs = jnp.where(core == 0, keep[1], keep[0])
        for n, unit in enumerate(units):
            where_own[unit] = (len(arrays), n)
        arrays.append(jnp.where(core == 0, keep[0], keep[1]))
        for kind in KINDS:
            chosen = [n for n, u in enumerate(units) if FAR[u[0]][2] == kind]
            for m, n in enumerate(chosen):
                where_other[units[n]] = (len(arrays), m)
            arrays.append(lax.ppermute(theirs[chosen[0] : chosen[-1] + 1], "occ", partner[kind]))

    spots = [(a, b) for a in range(blocks) for b in range(blocks)]
    tiles = []
    for name, (_, _, scale) in NEAR.items():
        parts = {(a, b): (*where_own[name, a, b], *where_other[name, a, b], False) for a, b in spots}
        tiles.append((1 + 5 * len(tiles), scale, "near", parts))
    for name, spec in FAR.items():
        parts = {(a, b): (*where_own[name, a, b], *where_other[spec[3], b, a], True) for a, b in spots}
        tiles.append((1 + 5 * len(tiles), 1.0, "far", parts))
    vir = vir_energies[None, :]

    def run(base, picked, slots):
        used = sorted({x for p in picked for t in p[3].values() for x in (t[0], t[2])})
        picked = [
            (*p[:3], {k: (used.index(t[0]), t[1], used.index(t[2]), *t[3:]) for k, t in p[3].items()}) for p in picked
        ]
        occ = []
        for name in slots:
            for o in range(CORES):
                start = CORES * VB + o * TAIL
                x = chunks[name, 0][start : start + 3, :LANES].astype(jnp.float32)
                occ.append((x[0:1] + x[1:2]) + x[2:3])
        occ = jnp.concatenate(occ, axis=0)
        return add_tiles(blocks, picked, row, aux, vir, occ, base, shape, [arrays[n] for n in used])

    table = run(None, tiles[: len(NEAR)], SLOTS[:4])
    return run(table, tiles[len(NEAR) :], SLOTS)


def sum_over(value, names):
    for name in names:
        size = lax.axis_size(name)
        if size & (size - 1):
            value = lax.psum(value, name)
            continue
        step = 1
        while step < size:
            value = value + lax.ppermute(value, name, [(k, k ^ step) for k in range(size)])
            step *= 2
    return value


def product(left, right):
    return lax.dot_general(left, right, (((1,), (1,)), ((), ())), preferred_element_type=jnp.float32)


def ring(order, panel, occ_all, vir_energies, table):
    virt, depth = panel.shape
    blocks = virt // VB
    occ_size, _ = table.shape
    aux_size = lax.axis_size("aux")
    me = lax.axis_index("occ")
    my_aux = lax.axis_index("aux")
    core = me % CORES
    chips = occ_size // CORES
    place = {c: k for k, c in enumerate(order)}

    share = depth // CORES
    swap = [(k, k ^ 1) for k in range(occ_size)]

    def turn(step):
        return [
            (c * CORES + k, order[(place[c] + step) % chips] * CORES + k)
            for c in range(chips)
            for k in range(CORES)
        ]

    kept = lax.dynamic_slice_in_dim(panel, core * share, share, 1)
    sent = lax.dynamic_slice_in_dim(panel, (1 - core) * share, share, 1)
    got = lax.ppermute(sent, "occ", swap)
    home = [kept[b * VB : (b + 1) * VB] for b in range(blocks)]
    home += [got[b * VB : (b + 1) * VB] for b in range(blocks)]

    hops = -(-(chips // 2) // 2)
    held = {0: home}
    up, down = turn(1), turn(-1)
    for hop in range(1, hops + 1):
        below, above = [], []
        for k in range(len(home)):
            below.append(lax.ppermute(held[1 - hop][k], "occ", up))
            above.append(lax.ppermute(held[hop - 1][k], "occ", down))
        held[-hop], held[hop] = below, above
    slabs = {k: jnp.concatenate(v, axis=0) for k, v in held.items()}

    ring_ids = jnp.asarray(
        np.array([[order[(place[c] + o) % chips] for o in range(-hops, hops + 1)] for c in range(chips)], np.int32)
    )[me // CORES]
    virt_col = jnp.broadcast_to(vir_energies[:, None], (virt, LANES))
    virt_row = jnp.broadcast_to(vir_energies[None, :], (8, virt))

    def work(distance):
        a = -(distance // 2)
        b = a + distance
        whole = product(slabs[a], slabs[b])
        other = lax.ppermute(whole[virt:], "occ", swap)
        weight = 0.5 if distance == 0 or 2 * distance == chips else 1.0
        own = [whole[:virt, :virt], whole[:virt, virt:]]
        other = [other[:, virt:], other[:, :virt]]
        i = ring_ids[a + hops] * CORES + core
        js = [ring_ids[b + hops] * CORES + core, ring_ids[b + hops] * CORES + 1 - core]
        both = [x + y for x, y in zip(own, other)]
        if aux_size == 2:
            first = my_aux == 0
            keep = jnp.where(first, both[0], both[1])
            send = jnp.where(first, both[1], both[0])
            return [(i, jnp.where(first, js[0], js[1]), weight, keep, lax.ppermute(send, "aux", [(0, 1), (1, 0)]))]
        both = [lax.psum(x, "aux") for x in both]
        return [(i, j, weight / aux_size, x, jnp.zeros_like(x)) for j, x in zip(js, both)]

    distances = list(range(chips // 2 + 1))
    early = [d for d in distances if d <= 2 * (hops - 1)]
    late = [d for d in distances if d not in early]
    for group in (early, late):
        done = [x for d in group for x in work(d)]
        ids = jnp.stack([jnp.stack([x[0], x[1]]) for x in done]).astype(jnp.int32)
        weights = jnp.asarray(np.array([x[2] for x in done], np.float32))
        first = jnp.stack([x[3] for x in done])
        second = jnp.stack([x[4] for x in done])
        table = add_energies(blocks, ids, occ_all, virt_col, virt_row, weights, first, second, table)
    return table


def local(order, grid, b_factors, occ_energies, vir_energies, pair_list, pair_count):
    panel = b_factors[0]
    virt, _ = panel.shape
    blocks = virt // VB
    occ_size = lax.axis_size("occ")
    aux_size = lax.axis_size("aux")
    me = lax.axis_index("occ")
    my_aux = lax.axis_index("aux")

    items = pair_list[0]
    slots = items.shape[0]
    codes = (items[:, 0] * blocks + items[:, 1]) * blocks + items[:, 2]
    live = jnp.arange(slots, dtype=jnp.int32) < pair_count[0]
    span = occ_size * blocks * blocks
    width = -(-2 * span // LANES) * LANES
    code_ids = jnp.arange(span, dtype=jnp.int32)
    listed = jnp.sum(((codes[:, None] == code_ids[None, :]) & live[:, None]).astype(jnp.float32), axis=0)
    mine = (jnp.arange(occ_size, dtype=jnp.int32) == me)[:, None]
    if grid is not None and aux_size == 2:
        table = two_way(grid, panel, occ_energies, vir_energies, (occ_size, width))
    else:
        occ_all = jnp.where(jnp.arange(occ_size, dtype=jnp.int32) == me, occ_energies[0], 0.0)
        occ_all = sum_over(occ_all[None, :], ["occ"])[0]
        table = ring(order, panel, occ_all, vir_energies, jnp.zeros((occ_size, width), jnp.float32))
    shown = jnp.where(mine & (my_aux == 0), listed[None, :], 0.0)
    table = table + jnp.pad(shown, ((0, 0), (span, width - 2 * span)))
    table = sum_over(table, ["occ", "aux"])
    listed_all = table[:, span : 2 * span]
    table = table[:, :span]

    per_device = slots // aux_size
    my_codes = lax.dynamic_slice_in_dim(codes, my_aux * per_device, per_device, 0)
    my_live = lax.dynamic_slice_in_dim(live, my_aux * per_device, per_device, 0)
    row = jnp.sum(jnp.where(mine, table, 0.0), axis=0)
    energy = jnp.sum(jnp.where(my_codes[:, None] == code_ids[None, :], row[None, :], 0.0), axis=1)
    energy = jnp.where(my_live, energy, 0.0)
    total = jnp.sum(table * listed_all)
    return energy[None, :], total


def solution(mesh):
    return jax.shard_map(
        functools.partial(local, ring_order(mesh), grid_of(mesh)),
        mesh=mesh,
        in_specs=(P("occ", None, "aux"), P("occ"), P(), P("occ", None, None), P("occ")),
        out_specs=(P("occ", "aux"), P()),
        check_vma=False,
    )
```

```python
import functools

import jax
import jax.numpy as jnp
import numpy as np
from jax import lax
from jax.experimental import pallas as pl
from jax.experimental.pallas import tpu as pltpu
from jax.sharding import PartitionSpec as P

VB = 128
CORES = 2
LANES = 128


def ring_order(mesh):
    devices = mesh.devices[:, 0]
    chips = len(devices) // CORES
    plain = list(range(chips))
    places = [getattr(d, "coords", None) for d in devices[::CORES]]
    if any(p is None for p in places) or len(set(map(tuple, places))) != chips:
        return plain
    at = {tuple(p): k for k, p in enumerate(places)}
    axes = [sorted({p[d] for p in places}) for d in range(len(places[0]))]
    long = [d for d, values in enumerate(axes) if len(values) > 1]
    if len(long) != 2 or len(axes[long[0]]) * len(axes[long[1]]) != chips:
        return plain
    u, v = sorted(long, key=lambda d: len(axes[d]) % 2)
    if len(axes[u]) % 2:
        return plain

    def chip(i, j):
        place = list(places[0])
        place[u], place[v] = axes[u][i], axes[v][j]
        return at[tuple(place)]

    rows, columns = len(axes[u]), len(axes[v])
    order = []
    for i in range(rows):
        inner = range(1, columns) if i % 2 == 0 else range(columns - 1, 0, -1)
        order += [chip(i, j) for j in inner]
    return order + [chip(i, 0) for i in range(rows - 1, -1, -1)]


def energy_kernel(blocks, ids_ref, occ_ref, vcol_ref, vrow_ref, weight_ref, first_ref, second_ref, base_ref, table_ref):
    rows = lax.broadcasted_iota(jnp.int32, table_ref.shape, 0)
    columns = lax.broadcasted_iota(jnp.int32, table_ref.shape, 1)
    table = base_ref[...]
    pair_sum = vcol_ref[:, :1] + vrow_ref[:1, :]
    for m in range(first_ref.shape[0]):
        i = ids_ref[m, 0]
        j = ids_ref[m, 1]
        tile = first_ref[m] + second_ref[m]
        denominator = pair_sum - occ_ref[i] - occ_ref[j]
        terms = tile * (2.0 * tile - jnp.transpose(tile)) / denominator
        for a in range(blocks):
            line = jnp.sum(terms[a * VB : (a + 1) * VB], axis=0, keepdims=True)
            for b in range(blocks):
                value = -weight_ref[m] * jnp.sum(line[:, b * VB : (b + 1) * VB], axis=1, keepdims=True)
                here = (rows == i) & (columns == (j * blocks + a) * blocks + b)
                there = (rows == j) & (columns == (i * blocks + b) * blocks + a)
                table += jnp.where(here, value, 0.0) + jnp.where(there, value, 0.0)
    table_ref[...] = table


def add_energies(blocks, ids, occ, vcol, vrow, weights, first, second, base):
    smem = pl.BlockSpec(memory_space=pltpu.SMEM)
    vmem = pl.BlockSpec(memory_space=pltpu.VMEM)
    return pl.pallas_call(
        functools.partial(energy_kernel, blocks),
        out_shape=jax.ShapeDtypeStruct(base.shape, jnp.float32),
        in_specs=[smem, smem, vmem, vmem, smem, vmem, vmem, vmem],
        out_specs=vmem,
        cost_estimate=pl.CostEstimate(
            flops=20 * first.size, bytes_accessed=8 * first.size, transcendentals=0
        ),
    )(ids, occ, vcol, vrow, weights, first, second, base)


NEAR = {
    "HH": ("H", "H", 0.5),
    "HB": ("H", "B", 1.0),
    "HX": ("H", "X", 0.5),
    "BA": ("B", "A", 1.0),
    "BX": ("B", "X", 1.0),
}
FAR = {
    "FU": ("F", "U", "same", "FU"),
    "FX": ("F", "X", "cross", "LG"),
    "LG": ("L", "G", "cross", "FX"),
    "FG": ("F", "G", "cross", "FG"),
}
KINDS = ("same", "cross")
SLOTS = ("H", "X", "L", "U", "F", "G")
TAIL = 8


def grid_of(mesh):
    devices = mesh.devices[:, 0]
    places = [getattr(d, "coords", None) for d in devices[::CORES]]
    if any(p is None for p in places) or len(devices) % CORES:
        return None
    axes = [sorted({p[d] for p in places}) for d in range(len(places[0]))]
    long = sorted((d for d, v in enumerate(axes) if len(v) > 1), key=lambda d: len(axes[d]))
    if [len(axes[d]) for d in long] != [2, 4] or len(set(map(tuple, places))) != len(places):
        return None
    return [(axes[long[0]].index(p[long[0]]), axes[long[1]].index(p[long[1]])) for p in places]


def split_kernel(block, core_ref, energy_ref, panel_ref, kept_ref, sent_ref, sems):
    rows, share = kept_ref.shape
    core = core_ref[0]
    copies = []
    for n, (target, part) in enumerate(((sent_ref, CORES - 1 - core), (kept_ref, core))):
        start = pl.multiple_of(part * share, LANES)
        source = panel_ref.at[pl.ds(block * VB, VB), pl.ds(start, share)]
        copies.append(pltpu.make_async_copy(source, target.at[pl.ds(0, rows)], sems.at[n]))
        copies[-1].start()
    below = sent_ref.shape[0] - rows
    if below:
        line = lax.broadcasted_iota(jnp.int32, (below, LANES), 0)
        rest = jnp.full((below, LANES), energy_ref[0], jnp.float32)
        tail = jnp.zeros_like(rest)
        for n in range(3):
            term = rest.astype(jnp.bfloat16).astype(jnp.float32)
            tail = jnp.where(line == n, term, tail)
            rest = rest - term
        sent_ref[rows:, :LANES] = tail.astype(sent_ref.dtype)
        sent_ref[rows:, LANES:] = jnp.zeros((below, share - LANES), sent_ref.dtype)
    for copy in copies:
        copy.wait()


def split(panel, block, core, energy, share):
    smem = pl.BlockSpec(memory_space=pltpu.SMEM)
    vmem = pl.BlockSpec(memory_space=pltpu.VMEM)
    below = TAIL if block == 0 else 0
    return pl.pallas_call(
        functools.partial(split_kernel, block),
        out_shape=(
            jax.ShapeDtypeStruct((VB, share), panel.dtype),
            jax.ShapeDtypeStruct((VB + below, share), panel.dtype),
        ),
        in_specs=[smem, smem, pl.BlockSpec(memory_space=pltpu.HBM)],
        out_specs=(vmem, vmem),
        scratch_shapes=[pltpu.SemaphoreType.DMA((2,))],
    )(core, energy, panel)


def product_kernel(steps, picks, row_ref, aux_ref, *refs):
    if picks > 1:
        own_ref, over_ref, mid_ref, first_ref, second_ref = refs[-5:]
    else:
        keep_ref, send_ref = refs[-2:]
    core = row_ref[0, 0]
    aux = aux_ref[0]
    diag = (aux + core) % CORES == 0
    plain = aux == 0

    def run(left, right, unit):
        block = lax.dot_general(
            refs[left][: CORES * VB], refs[right][: CORES * VB], (((1,), (1,)), ((), ())), preferred_element_type=jnp.float32
        )
        half = VB
        t00, t01 = block[:half, :half], block[:half, half:]
        t10, t11 = block[half:, :half], block[half:, half:]
        if picks > 1:
            alike, unlike = jnp.where(diag, t00, t11), jnp.where(diag, t11, t00)
            kept, sent = jnp.where(plain, t10, t01), jnp.where(plain, t01, t10)
            upward = core == 0
            own_ref[unit] = jnp.where(upward, alike, kept)
            over_ref[unit] = jnp.where(upward, unlike, sent)
            mid_ref[unit] = jnp.where(upward, kept, alike)
            both_ref, place = (first_ref, unit) if unit < picks else (second_ref, unit - picks)
            both_ref[place] = jnp.where(upward, sent, unlike)
        elif picks:
            keep_ref[0, unit] = jnp.where(diag, t00, t11)
            send_ref[0, unit] = jnp.where(diag, t11, t00)
            keep_ref[1, unit] = jnp.where(plain, t10, t01)
            send_ref[1, unit] = jnp.where(plain, t01, t10)
        else:
            keep_ref[0, unit], keep_ref[1, unit] = t00, t01
            send_ref[0, unit], send_ref[1, unit] = t11, t10

    for unit, options in enumerate(steps):
        if len(options) == 1:
            run(*options[0], unit)
        else:
            for k, option in enumerate(options):
                pl.when(core == k)(functools.partial(run, *option, unit))


def products(units, chunks, row, aux, picks):
    arrays, places, steps = [], {}, []

    def place(name):
        if name not in places:
            places[name] = len(arrays)
            arrays.append(chunks[name])
        return places[name]

    for unit in units:
        options = []
        for k in range(CORES):
            option = tuple(place(chunks[c][k] if isinstance(chunks[c], tuple) else c) for c in unit)
            options += [option] if option not in options else []
        steps.append(options)
    rows, depth = CORES * VB, arrays[0].shape[1]
    count = len(units)
    dims = [(2, count, VB, VB)] * 2
    if picks > 1:
        dims = [(n, VB, VB) for n in (count, count, count, picks, count - picks)]
    smem = pl.BlockSpec(memory_space=pltpu.SMEM)
    vmem = pl.BlockSpec(memory_space=pltpu.VMEM)
    return pl.pallas_call(
        functools.partial(product_kernel, steps, picks),
        out_shape=tuple(jax.ShapeDtypeStruct(d, jnp.float32) for d in dims),
        in_specs=[smem, smem] + [vmem] * len(arrays),
        out_specs=(vmem,) * len(dims),
        compiler_params=pltpu.CompilerParams(vmem_limit_bytes=(44 if picks else 30) << 20),
        cost_estimate=pl.CostEstimate(
            flops=2 * rows * rows * depth * count, bytes_accessed=2 * len(arrays) * rows * depth, transcendentals=0
        ),
    )(row, aux, *arrays)


def tile_kernel(blocks, tiles, based, held, row_ref, aux_ref, vir_ref, *refs):
    table_ref, lines, occ_ref, sems = refs[-4:]
    copies = [
        pltpu.make_async_copy(
            refs[n].at[pl.ds(CORES * VB, CORES * TAIL), pl.ds(0, LANES)], lines.at[n], sems.at[n]
        )
        for n in range(held)
    ]
    for copy in copies:
        copy.start()
    arrays = refs[held + 1 : -4] if based else refs[held:-4]
    rows = lax.broadcasted_iota(jnp.int32, table_ref.shape, 0)
    columns = lax.broadcasted_iota(jnp.int32, table_ref.shape, 1)
    table = refs[held][...] if based else jnp.zeros(table_ref.shape, jnp.float32)
    for copy in copies:
        copy.wait()
    for n in range(held):
        x = lines[n].astype(jnp.float32)
        for o in range(CORES):
            t = o * TAIL
            occ_ref[n * CORES + o : n * CORES + o + 1, :] = (x[t : t + 1] + x[t + 1 : t + 2]) + x[t + 2 : t + 3]
    aux, core = aux_ref[0], row_ref[0, 0]
    mixed = (aux + core) % CORES
    line = [vir_ref[:, a * VB : (a + 1) * VB] for a in range(blocks)]
    tall = [jnp.transpose(jnp.broadcast_to(x, (VB, VB))) for x in line]
    for place, scale, sides, parts in tiles:
        offset = {"far": (aux, mixed), "near": (core, mixed)}[sides]
        i = row_ref[0, place] * CORES + offset[0]
        j = row_ref[0, place + 1] * CORES + offset[1]
        left_energy = occ_ref[pl.ds(row_ref[0, place + 3] * CORES + (offset[0] + core) % CORES, 1), :]
        right_energy = occ_ref[pl.ds(row_ref[0, place + 4] * CORES + (offset[1] + core) % CORES, 1), :]
        weight = row_ref[0, place + 2].astype(jnp.float32) * -scale
        tile = {}
        for key, (ones, twos, turned) in parts.items():
            other = functools.reduce(jnp.add, [arrays[n][u] for n, u in twos])
            this = functools.reduce(jnp.add, [arrays[n][u] for n, u in ones])
            tile[key] = this + (jnp.transpose(other) if turned else other)
        for a in range(blocks):
            for b in range(blocks):
                denominator = (tall[a] + line[b]) - left_energy - right_energy
                terms = tile[a, b] * (2.0 * tile[a, b] - jnp.transpose(tile[b, a])) / denominator
                value = weight * jnp.sum(jnp.sum(terms, axis=0, keepdims=True), axis=1, keepdims=True)
                here = (rows == i) & (columns == (j * blocks + a) * blocks + b)
                there = (rows == j) & (columns == (i * blocks + b) * blocks + a)
                table += jnp.where(here, value, 0.0) + jnp.where(there, value, 0.0)
    table_ref[...] = table


def add_tiles(blocks, tiles, row, aux, vir, held, base, shape, arrays):
    smem = pl.BlockSpec(memory_space=pltpu.SMEM)
    vmem = pl.BlockSpec(memory_space=pltpu.VMEM)
    given = [] if base is None else [base]
    size = len(tiles) * (blocks * VB) ** 2
    return pl.pallas_call(
        functools.partial(tile_kernel, blocks, tiles, base is not None, len(held)),
        out_shape=jax.ShapeDtypeStruct(shape, jnp.float32),
        in_specs=[smem, smem, vmem]
        + [pl.BlockSpec(memory_space=pl.ANY)] * len(held)
        + [vmem] * (len(given) + len(arrays)),
        out_specs=vmem,
        scratch_shapes=[
            pltpu.VMEM((len(held), CORES * TAIL, LANES), jnp.bfloat16),
            pltpu.VMEM((2 * len(held) + 4, LANES), jnp.float32),
            pltpu.SemaphoreType.DMA((len(held),)),
        ],
        compiler_params=pltpu.CompilerParams(vmem_limit_bytes=16 << 20),
        cost_estimate=pl.CostEstimate(flops=40 * size, bytes_accessed=8 * size, transcendentals=0),
    )(row, aux, vir, *held, *given, *arrays)


def two_way(grid, panel, my_energy, vir_energies, shape):
    virt, depth = panel.shape
    blocks = virt // VB
    occ_size = lax.axis_size("occ")
    aux_size = lax.axis_size("aux")
    me = lax.axis_index("occ")
    my_aux = lax.axis_index("aux")
    core = me % CORES
    share = depth // CORES
    chip_at = {p: c for c, p in enumerate(grid)}
    last = max(p[1] for p in grid)

    def row_of(role, k):
        return role if k == 0 else last - role

    def device(u, role, k):
        return chip_at[u, row_of(role, k)] * CORES + k

    every = [(u, k) for u in range(2) for k in range(CORES)]
    ahead = [(device(u, r, k), device(u, r + 1, k)) for u, k in every for r in range(last)]
    back = [(device(u, r + 1, k), device(u, r, k)) for u, k in every for r in range(last)]
    across = [(device(u, r, k), device(1 - u, r, k)) for u, k in every for r in range(last + 1)]
    far_ahead = [(device(u, 1, k), device(u, 2, k)) for u, k in every]
    far_across = [(device(u, 2, k), device(1 - u, 2, k)) for u, k in every]
    swap = [(k, k ^ 1) for k in range(occ_size)]
    centres = sorted(device(u, 2, k) for u, k in every)
    over_aux = [(d * aux_size + y, d * aux_size + 1 - y) for d in centres for y in range(aux_size)]
    all_aux = [(y, 1 - y) for y in range(aux_size)]
    partner = {
        "same": [(device(u, 2, k), device(u, 2, 1 - k)) for u, k in every],
        "cross": [(device(u, 2, k), device(1 - u, 2, 1 - k)) for u, k in every],
    }

    cores = jnp.reshape(core, (1,)).astype(jnp.int32)
    chunks = {}
    for b in range(blocks):
        kept, sent = split(panel, b, cores, my_energy, share)
        got = lax.ppermute(sent, "occ", swap)
        pieces = [kept, got[:VB], sent[VB:], got[VB:]] if b == 0 else [kept, got]
        home = jnp.concatenate(pieces, axis=0)
        chunks["H", b] = home
        chunks["L", b] = lax.ppermute(home, "occ", ahead)
        chunks["U", b] = lax.ppermute(home, "occ", back)
        chunks["X", b] = lax.ppermute(home, "occ", across)
    for b in range(blocks):
        chunks["F", b] = lax.ppermute(chunks["L", b], "occ", far_ahead)
        chunks["G", b] = lax.ppermute(chunks["U", b], "occ", far_across)
        chunks["B", b] = (("L", b), ("U", b))
        chunks["A", b] = (("U", b), ("L", b))

    facts = []
    for d in range(occ_size):
        (u, v), k = grid[d // CORES], d % CORES
        r = row_of(v, k)
        places = {"H": (u, v), "B": (u, v - 1), "A": (u, v + 1), "X": (1 - u, v)}
        places |= {"F": (u, row_of(0, k)), "L": (u, row_of(1, k)), "U": (u, row_of(3, k)), "G": (1 - u, row_of(3, k))}
        line = [k]
        slot = {n: n for n in SLOTS} | {"B": "LU"[k], "A": "UL"[k]}
        for table in (NEAR, FAR):
            for left, right in [x[:2] for x in table.values()]:
                good = places[left] in chip_at and places[right] in chip_at if table is NEAR else r == 2
                line += [chip_at.get(places[left], 0), chip_at.get(places[right], 0), int(good)]
                line += [SLOTS.index(slot[left]), SLOTS.index(slot[right])]
        facts.append(line)
    row = lax.dynamic_slice_in_dim(jnp.asarray(np.array(facts, np.int32)), me, 1, 0)
    aux = jnp.reshape(my_aux, (1,)).astype(jnp.int32)

    def at(name, b):
        return {"H": 0, "F": blocks + b, "G": blocks + b}.get(name, b)

    arrays, where_own, where_other = [], {}, {}

    def units_of(table, event):
        return [
            (name, a, b)
            for name, spec in table.items()
            for a in range(blocks)
            for b in range(blocks)
            if max(at(spec[0], a), at(spec[1], b)) == event
        ]

    upper = my_aux == 0
    for event in range(blocks):
        units = units_of(NEAR, event)
        work = [((NEAR[name][0], a), (NEAR[name][1], b)) for name, a, b in units]
        keep, send = products(work, chunks, row, aux, False)
        keep = keep + lax.ppermute(send, "occ", swap)
        other = lax.ppermute(jnp.where(upper, keep[1], keep[0]), "aux", all_aux)
        for n, unit in enumerate(units):
            where_own[unit] = (len(arrays), n)
            where_other[unit] = (len(arrays) + 1, n)
        arrays += [jnp.where(upper, keep[0], keep[1]), other]
    to_send, where_waiting = {kind: [] for kind in KINDS}, {kind: [] for kind in KINDS}
    for event in range(blocks, 2 * blocks):
        units = sorted(units_of(FAR, event), key=lambda u: KINDS.index(FAR[u[0]][2]))
        work = [((FAR[name][0], a), (FAR[name][1], b)) for name, a, b in units]
        if event == 2 * blocks - 1:
            cut = sum(FAR[u[0]][2] == KINDS[0] for u in units)
            own, over, mid, *both = products(work, chunks, row, aux, cut)
            for n, unit in enumerate(units):
                where_own[unit] = (len(arrays), n, len(arrays) + 1, n)
            arrays += [own, lax.ppermute(over, ("occ", "aux"), over_aux)]
            for k, kind in enumerate(KINDS):
                chosen = [n for n, u in enumerate(units) if FAR[u[0]][2] == kind]
                turned = [
                    (d * aux_size + y, e * aux_size + 1 - y) for d, e in partner[kind] for y in range(aux_size)
                ]
                waiting = where_waiting[kind]
                for m, unit in enumerate(waiting):
                    where_other[unit] = (len(arrays), m)
                for m, n in enumerate(chosen):
                    where_other[units[n]] = (len(arrays), len(waiting) + m, len(arrays) + 1, m)
                moved = lax.ppermute(both[k], ("occ", "aux"), turned)
                pieces = to_send[kind] + [mid[chosen[0] : chosen[-1] + 1]]
                arrays += [lax.ppermute(jnp.concatenate(pieces, axis=0), "occ", partner[kind]), moved]
            continue
        keep, send = products(work, chunks, row, aux, True)
        keep = keep + lax.ppermute(send, ("occ", "aux"), over_aux)
        theirs = jnp.where(core == 0, keep[1], keep[0])
        for n, unit in enumerate(units):
            where_own[unit] = (len(arrays), n)
        arrays.append(jnp.where(core == 0, keep[0], keep[1]))
        for kind in KINDS:
            chosen = [n for n, u in enumerate(units) if FAR[u[0]][2] == kind]
            to_send[kind].append(theirs[chosen[0] : chosen[-1] + 1])
            where_waiting[kind] += [units[n] for n in chosen]

    def couples(line):
        return [tuple(line[n : n + 2]) for n in range(0, len(line), 2)]

    spots = [(a, b) for a in range(blocks) for b in range(blocks)]
    tiles = []
    for name, (_, _, scale) in NEAR.items():
        parts = {(a, b): (couples(where_own[name, a, b]), couples(where_other[name, a, b]), False) for a, b in spots}
        tiles.append((1 + 5 * len(tiles), scale, "near", parts))
    for name, spec in FAR.items():
        parts = {(a, b): (couples(where_own[name, a, b]), couples(where_other[spec[3], b, a]), True) for a, b in spots}
        tiles.append((1 + 5 * len(tiles), 1.0, "far", parts))
    vir = vir_energies[None, :]

    def run(base, picked, slots):
        used = sorted({x for p in picked for t in p[3].values() for x, _ in t[0] + t[1]})
        picked = [
            (*p[:3], {k: (*[[(used.index(x), n) for x, n in c] for c in t[:2]], t[2]) for k, t in p[3].items()})
            for p in picked
        ]
        held = [chunks[name, 0] for name in slots]
        return add_tiles(blocks, picked, row, aux, vir, held, base, shape, [arrays[n] for n in used])

    table = run(None, tiles[: len(NEAR)], SLOTS[:4])
    return run(table, tiles[len(NEAR) :], SLOTS)


def sum_over(value, names):
    for name in names:
        size = lax.axis_size(name)
        if size & (size - 1):
            value = lax.psum(value, name)
            continue
        step = 1
        while step < size:
            value = value + lax.ppermute(value, name, [(k, k ^ step) for k in range(size)])
            step *= 2
    return value


def product(left, right):
    return lax.dot_general(left, right, (((1,), (1,)), ((), ())), preferred_element_type=jnp.float32)


def ring(order, panel, occ_all, vir_energies, table):
    virt, depth = panel.shape
    blocks = virt // VB
    occ_size, _ = table.shape
    aux_size = lax.axis_size("aux")
    me = lax.axis_index("occ")
    my_aux = lax.axis_index("aux")
    core = me % CORES
    chips = occ_size // CORES
    place = {c: k for k, c in enumerate(order)}

    share = depth // CORES
    swap = [(k, k ^ 1) for k in range(occ_size)]

    def turn(step):
        return [
            (c * CORES + k, order[(place[c] + step) % chips] * CORES + k)
            for c in range(chips)
            for k in range(CORES)
        ]

    kept = lax.dynamic_slice_in_dim(panel, core * share, share, 1)
    sent = lax.dynamic_slice_in_dim(panel, (1 - core) * share, share, 1)
    got = lax.ppermute(sent, "occ", swap)
    home = [kept[b * VB : (b + 1) * VB] for b in range(blocks)]
    home += [got[b * VB : (b + 1) * VB] for b in range(blocks)]

    hops = -(-(chips // 2) // 2)
    held = {0: home}
    up, down = turn(1), turn(-1)
    for hop in range(1, hops + 1):
        below, above = [], []
        for k in range(len(home)):
            below.append(lax.ppermute(held[1 - hop][k], "occ", up))
            above.append(lax.ppermute(held[hop - 1][k], "occ", down))
        held[-hop], held[hop] = below, above
    slabs = {k: jnp.concatenate(v, axis=0) for k, v in held.items()}

    ring_ids = jnp.asarray(
        np.array([[order[(place[c] + o) % chips] for o in range(-hops, hops + 1)] for c in range(chips)], np.int32)
    )[me // CORES]
    virt_col = jnp.broadcast_to(vir_energies[:, None], (virt, LANES))
    virt_row = jnp.broadcast_to(vir_energies[None, :], (8, virt))

    def work(distance):
        a = -(distance // 2)
        b = a + distance
        whole = product(slabs[a], slabs[b])
        other = lax.ppermute(whole[virt:], "occ", swap)
        weight = 0.5 if distance == 0 or 2 * distance == chips else 1.0
        own = [whole[:virt, :virt], whole[:virt, virt:]]
        other = [other[:, virt:], other[:, :virt]]
        i = ring_ids[a + hops] * CORES + core
        js = [ring_ids[b + hops] * CORES + core, ring_ids[b + hops] * CORES + 1 - core]
        both = [x + y for x, y in zip(own, other)]
        if aux_size == 2:
            first = my_aux == 0
            keep = jnp.where(first, both[0], both[1])
            send = jnp.where(first, both[1], both[0])
            return [(i, jnp.where(first, js[0], js[1]), weight, keep, lax.ppermute(send, "aux", [(0, 1), (1, 0)]))]
        both = [lax.psum(x, "aux") for x in both]
        return [(i, j, weight / aux_size, x, jnp.zeros_like(x)) for j, x in zip(js, both)]

    distances = list(range(chips // 2 + 1))
    early = [d for d in distances if d <= 2 * (hops - 1)]
    late = [d for d in distances if d not in early]
    for group in (early, late):
        done = [x for d in group for x in work(d)]
        ids = jnp.stack([jnp.stack([x[0], x[1]]) for x in done]).astype(jnp.int32)
        weights = jnp.asarray(np.array([x[2] for x in done], np.float32))
        first = jnp.stack([x[3] for x in done])
        second = jnp.stack([x[4] for x in done])
        table = add_energies(blocks, ids, occ_all, virt_col, virt_row, weights, first, second, table)
    return table


def local(order, grid, b_factors, occ_energies, vir_energies, pair_list, pair_count):
    panel = b_factors[0]
    virt, _ = panel.shape
    blocks = virt // VB
    occ_size = lax.axis_size("occ")
    aux_size = lax.axis_size("aux")
    me = lax.axis_index("occ")
    my_aux = lax.axis_index("aux")

    items = pair_list[0]
    slots = items.shape[0]
    codes = (items[:, 0] * blocks + items[:, 1]) * blocks + items[:, 2]
    live = jnp.arange(slots, dtype=jnp.int32) < pair_count[0]
    span = occ_size * blocks * blocks
    width = -(-2 * span // LANES) * LANES
    code_ids = jnp.arange(span, dtype=jnp.int32)
    listed = jnp.sum(((codes[:, None] == code_ids[None, :]) & live[:, None]).astype(jnp.float32), axis=0)
    mine = (jnp.arange(occ_size, dtype=jnp.int32) == me)[:, None]
    if grid is not None and aux_size == 2:
        table = two_way(grid, panel, occ_energies, vir_energies, (occ_size, width))
    else:
        occ_all = jnp.where(jnp.arange(occ_size, dtype=jnp.int32) == me, occ_energies[0], 0.0)
        occ_all = sum_over(occ_all[None, :], ["occ"])[0]
        table = ring(order, panel, occ_all, vir_energies, jnp.zeros((occ_size, width), jnp.float32))
    shown = jnp.where(mine & (my_aux == 0), listed[None, :], 0.0)
    table = table + jnp.pad(shown, ((0, 0), (span, width - 2 * span)))
    table = sum_over(table, ["occ", "aux"])
    listed_all = table[:, span : 2 * span]
    table = table[:, :span]

    per_device = slots // aux_size
    my_codes = lax.dynamic_slice_in_dim(codes, my_aux * per_device, per_device, 0)
    my_live = lax.dynamic_slice_in_dim(live, my_aux * per_device, per_device, 0)
    row = jnp.sum(jnp.where(mine, table, 0.0), axis=0)
    energy = jnp.sum(jnp.where(my_codes[:, None] == code_ids[None, :], row[None, :], 0.0), axis=1)
    energy = jnp.where(my_live, energy, 0.0)
    total = jnp.sum(table * listed_all)
    return energy[None, :], total


def solution(mesh):
    return jax.shard_map(
        functools.partial(local, ring_order(mesh), grid_of(mesh)),
        mesh=mesh,
        in_specs=(P("occ", None, "aux"), P("occ"), P(), P("occ", None, None), P("occ")),
        out_specs=(P("occ", "aux"), P()),
        check_vma=False,
    )
```
